32 devices in a mesh: row: 4 (over x, core), col: 8 (over z, y).
Axes of the slice: x: 2, y: 2, z: 4, core: 2. Of those that a mesh axis runs over, the one named last changes fastest.
Arguments:
- left_factor: bfloat16 [4096, 2048], P('row', 'col'), may hold values from -6 to 6
- right_factor: bfloat16 [2048, 8192], P('row', 'col'), may hold values from -0.125 to 0.125
- matrix: float32 [4096, 8192], P('row', 'col'), may hold values from -6 to 6
- pivot_scale: float32 [2048], replicated, may hold values from 0.25 to 1.75
Outputs:
- updated: float32 [4096, 8192], P('row', 'col')
The draws below stay inside these ranges and needn't reach their ends.
All inputs are finite; a program needn't handle non-finite values.
Results may differ from the reference program's by a relative error of at most 0.0003.
Values may be sent and summed in bfloat16 or wider, within the bound.
A program may use at most 128 MiB of HBM per device.

```python
import jax
import jax.numpy as jnp
from jax import lax

ROWS = 4096
COLS = 8192
INNER = 2048


def levels(rng, shape, split, least, top_value):
    def one(position, blocks):
        draws = jax.random.uniform(jax.random.fold_in(jax.random.fold_in(rng, 6), position), (blocks,), jnp.float32, least / len(split), top_value / len(split))
        return jnp.repeat(jnp.exp(draws), shape[position] // blocks).reshape((-1,) + (1,) * (len(shape) - position - 1))

    factor_of = one(*split[0])
    for cut in split[1:]:
        factor_of = factor_of * one(*cut)
    return factor_of


def scatter_about(stream_key, shape, spread, reach, split=(), held_as=jnp.bfloat16):
    gain = levels(stream_key, shape, split, -0.22, 0.18) if split else 1.0
    array = jax.random.normal(stream_key, shape, jnp.float32) * spread * gain
    return jnp.minimum(jnp.maximum(array, -reach), reach).astype(held_as)


def setup_inputs(seed: int = 0) -> dict:
    key_list = jax.random.split(jax.random.key(seed), 5)
    return {
        "left_factor": scatter_about(key_list[0], (ROWS, INNER), 1.0, 6.0, ((0, 4), (1, 8))),
        "right_factor": scatter_about(key_list[1], (INNER, COLS), INNER ** -0.5, 0.125, ((0, 4), (1, 8))),
        "matrix": scatter_about(key_list[2], (ROWS, COLS), 1.0, 6.0, ((0, 4), (1, 8)), jnp.float32),
        "pivot_scale": jnp.clip(1.0 + 0.15 * jax.random.normal(key_list[3], (INNER,), jnp.float32), 0.25, 1.75),
    }


def reference(left_factor, right_factor, matrix, pivot_scale):
    scaled_left = (left_factor.astype(jnp.float32) * pivot_scale).astype(jnp.bfloat16)
    updated = matrix - jnp.dot(scaled_left, right_factor, preferred_element_type=jnp.float32)
    row_power = lax.optimization_barrier(jnp.sum(updated * updated, axis=1))
    updated = updated * lax.rsqrt(row_power / COLS + 1e-06)[:, None]
    return updated
```

```python
import functools

import jax
import jax.numpy as jnp
from jax import lax
from jax.experimental import pallas as pl
from jax.experimental.pallas import tpu as pltpu
from jax.sharding import PartitionSpec as P

MESH = pl.DeviceIdType.MESH
STRIP = 128
PARTS = 4
UP, DOWN, ACROSS, RELAY = 0, 1, 2, 3


def kernel(
    n_row, n_col,
    left_hbm, right_hbm, matrix_hbm, scale_ref,
    out_ref, norm_ref,
    left, right, matrix, scaled, stats,
    left_send, left_recv, right_send, right_recv, stat_send, stat_recv, local_sem,
):
    rows, share = left_hbm.shape
    depth, cols = right_hbm.shape
    lines = n_col // 2
    strips = rows // STRIP
    part = depth // PARTS
    offset = max(lines, PARTS) - 1

    me = lax.axis_index("col")
    z, y = me // 2, me % 2
    z_pair = z + 1 - 2 * (z % 2)
    partner = z * 2 + 1 - y
    row = lax.axis_index("row")
    x, core = row // 2, row % 2
    sibling = x * 2 + 1 - core

    def strip_of(q):
        return pl.ds(pl.multiple_of(q * STRIP, STRIP), STRIP)

    def send_left(piece, q, to, way, own=False):
        return pltpu.make_async_remote_copy(
            src_ref=left_hbm.at[strip_of(q)] if own else left.at[piece, strip_of(q)],
            dst_ref=left.at[piece, strip_of(q)],
            send_sem=left_send.at[way, piece, q],
            recv_sem=left_recv.at[piece, q],
            device_id={"col": to},
            device_id_type=MESH,
        )

    def await_left(piece, q):
        send_left(piece, q, partner, ACROSS).wait_recv()

    def part_of(block, g):
        return pl.ds(pl.multiple_of(block * depth + g * part, part), part)

    def send_right(block, g, to, own=False):
        source = right_hbm.at[pl.ds(pl.multiple_of(g * part, part), part)]
        return pltpu.make_async_remote_copy(
            src_ref=source if own else right.at[part_of(block, g)],
            dst_ref=right.at[part_of(block, g)],
            send_sem=right_send.at[to, block, g],
            recv_sem=right_recv.at[block, g],
            device_id={"row": to},
            device_id_type=MESH,
        )

    def send_stat(c, to):
        return pltpu.make_async_remote_copy(
            src_ref=stats.at[me, c],
            dst_ref=stats.at[me, c],
            send_sem=stat_send.at[to, c],
            recv_sem=stat_recv.at[me, c],
            device_id={"col": to},
            device_id_type=MESH,
        )

    def await_stat(source, c):
        pltpu.make_async_remote_copy(
            src_ref=stats.at[source, c],
            dst_ref=stats.at[source, c],
            send_sem=stat_send.at[source, c],
            recv_sem=stat_recv.at[source, c],
            device_id={"col": source},
            device_id_type=MESH,
        ).wait_recv()

    own_left = pltpu.make_async_copy(left_hbm, left.at[me], local_sem.at[0])
    own_right = pltpu.make_async_copy(
        right_hbm, right.at[pl.ds(pl.multiple_of(row * depth, depth), depth)], local_sem.at[1]
    )
    own_matrix = pltpu.make_async_copy(matrix_hbm, matrix, local_sem.at[2])

    barrier = pltpu.get_barrier_semaphore()
    for step in range(1, n_col):
        pl.semaphore_signal(
            barrier, inc=1, device_id={"col": (me + step) % n_col}, device_id_type=MESH
        )
    far = [((x + step) % (n_row // 2)) * 2 + core for step in range(1, n_row // 2)]
    for other in far + [sibling]:
        pl.semaphore_signal(barrier, inc=1, device_id={"row": other}, device_id_type=MESH)
    own_left.start()
    own_right.start()
    own_matrix.start()
    pl.semaphore_wait(barrier, n_col - 1 + len(far) + 1)

    def own_sends(q, act):
        @pl.when(z < lines - 1)
        def _():
            act(send_left(me, q, me + 2, UP, own=True))

        @pl.when(z > 0)
        def _():
            act(send_left(me, q, me - 2, DOWN, own=True))

        act(send_left(me, q, partner, ACROSS, own=True))

    def passed_on(t, act, await_first):
        for d in range(1, lines):
            q = t - (d - 1)

            @pl.when((q >= 0) & (q < strips))
            def _():
                skip = (q % 2) == 1

                def cross(piece, z_from):
                    if d == 1:

                        @pl.when(jnp.logical_not((z_from == z_pair) & skip))
                        def _():
                            act(send_left(piece, q, partner, ACROSS))
                    else:
                        act(send_left(piece, q, partner, ACROSS))

                @pl.when(z + d < lines)
                def _():
                    piece = me + 2 * d
                    if await_first:
                        await_left(piece, q)

                    @pl.when(z > 0)
                    def _():
                        act(send_left(piece, q, me - 2, DOWN))

                    cross(piece, z + d)

                @pl.when(z - d >= 0)
                def _():
                    piece = me - 2 * d
                    if await_first:
                        await_left(piece, q)

                    @pl.when(z < lines - 1)
                    def _():
                        act(send_left(piece, q, me + 2, UP))

                    cross(piece, z - d)

        @pl.when((t < strips) & (t % 2 == 1))
        def _():
            if await_first:
                await_left(partner, t)
            act(send_left(partner, t, z_pair * 2 + y, RELAY))

    def start(copy):
        copy.start()

    def done(copy):
        copy.wait_send()

    @pl.loop(0, strips)
    def _(q):
        own_sends(q, start)

    @pl.loop(0, PARTS)
    def _(g):
        for other in far:
            send_right(row, g, other, own=True).start()
        send_right(row, g, sibling, own=True).start()

    def product(c):
        here = strip_of(c)
        for piece in range(n_col):
            span = slice(piece * share, (piece + 1) * share)
            scaled[:, span] = (
                left[piece, here, :].astype(jnp.float32) * scale_ref[:, span]
            ).astype(jnp.bfloat16)
        width = 256
        power = jnp.zeros((STRIP, 128), jnp.float32)

        def tile(n, power):
            span = pl.ds(pl.multiple_of(n * width, width), width)
            value = matrix[here, span] - jnp.dot(
                scaled[...], right[:, span], preferred_element_type=jnp.float32
            )
            out_ref[here, span] = value
            square = value * value
            for k in range(width // 128):
                power = power + square[:, k * 128 : (k + 1) * 128]
            return power

        power = lax.fori_loop(0, cols // width, tile, power)
        stats[me, c] = lax.dot_general(
            jnp.ones((8, 128), jnp.float32),
            power,
            (((1,), (1,)), ((), ())),
            precision=lax.Precision.HIGHEST,
            preferred_element_type=jnp.float32,
        )

    @pl.loop(0, strips + offset)
    def _(t):
        passed_on(t, start, True)

        @pl.when(t < PARTS)
        def _():
            for other in far:
                send_right(other, t, sibling).wait_recv()
                send_right(other, t, sibling).start()

        @pl.when(t == offset)
        def _():
            own_left.wait()
            own_right.wait()
            own_matrix.wait()

            @pl.loop(0, PARTS)
            def _(g):
                for step in range(n_row // 2):
                    send_right(step * 2 + 1 - core, g, sibling).wait_recv()

        c = t - offset

        @pl.when(c >= 0)
        def _():
            for line in range(lines):

                @pl.when(jnp.logical_not((line == z) & (c % 2 == 1)))
                def _():
                    await_left(line * 2 + 1 - y, c)

            product(c)
            for step in range(1, n_col):
                send_stat(c, (me + step) % n_col).start()

    @pl.loop(0, strips)
    def _(q):
        own_sends(q, done)

    @pl.loop(0, strips + lines - 2)
    def _(t):
        passed_on(t, done, False)

    @pl.loop(0, PARTS)
    def _(g):
        for other in far:
            send_right(row, g, other, own=True).wait_send()
            send_right(other, g, sibling).wait_send()
        send_right(row, g, sibling, own=True).wait_send()

    @pl.loop(0, strips)
    def _(c):
        for step in range(1, n_col):
            await_stat((me + step) % n_col, c)
            send_stat(c, (me + step) % n_col).wait_send()
        total = stats[0, c]
        for source in range(1, n_col):
            total = total + stats[source, c]
        norm_ref[c] = lax.rsqrt(total / (cols * n_col) + 1e-06)


def per_device(n_row, n_col, left_factor, right_factor, matrix, pivot_scale):
    rows, share = left_factor.shape
    depth, cols = right_factor.shape
    strips = rows // STRIP
    dma = pltpu.SemaphoreType.DMA
    updated, norm = pl.pallas_call(
        functools.partial(kernel, n_row, n_col),
        out_shape=(
            jax.ShapeDtypeStruct((rows, cols), jnp.float32),
            jax.ShapeDtypeStruct((strips, 8, STRIP), jnp.float32),
        ),
        in_specs=[pl.BlockSpec(memory_space=pl.ANY)] * 3
        + [pl.BlockSpec(memory_space=pltpu.VMEM)],
        out_specs=(
            pl.BlockSpec(memory_space=pltpu.VMEM),
            pl.BlockSpec(memory_space=pltpu.VMEM),
        ),
        scratch_shapes=[
            pltpu.VMEM((n_col, rows, share), jnp.bfloat16),
            pltpu.VMEM((n_row * depth, cols), jnp.bfloat16),
            pltpu.VMEM((rows, cols), jnp.float32),
            pltpu.VMEM((STRIP, n_col * share), jnp.bfloat16),
            pltpu.VMEM((n_col, strips, 8, STRIP), jnp.float32),
            dma((4, n_col, strips)),
            dma((n_col, strips)),
            dma((n_row, n_row, PARTS)),
            dma((n_row, PARTS)),
            dma((n_col, strips)),
            dma((n_col, strips)),
            dma((3,)),
        ],
        compiler_params=pltpu.CompilerParams(
            collective_id=0, has_side_effects=True, vmem_limit_bytes=60 * 1024 * 1024
        ),
    )(left_factor, right_factor, matrix, pivot_scale.reshape(1, -1))
    return updated * norm[:, 0, :].reshape(rows, 1)


def solution(mesh):
    in_specs = (P("row", "col"), P("row", "col"), P("row", "col"), P())
    out_specs = P("row", "col")
    body = functools.partial(per_device, mesh.shape["row"], mesh.shape["col"])
    return jax.shard_map(
        body, mesh=mesh, in_specs=in_specs, out_specs=out_specs, check_vma=False
    )
```
